32 devices in a mesh: sp: 4 (over z), tp: 8 (over y, x, core).
Axes of the slice: x: 2, y: 2, z: 4, core: 2. Of those that a mesh axis runs over, the one named last changes fastest.
Arguments:
- tokens: bfloat16 [8192, 2048], P(('sp', 'tp')), may hold values from -3 to 3
- queries: bfloat16 [8192, 2048], P(('sp', 'tp')), may hold values from -140 to 140
- keys: bfloat16 [8192, 1024], P(('sp', 'tp')), may hold values from -6 to 6
- values: bfloat16 [8192, 1024], P(('sp', 'tp')), may hold values from -6 to 6
- out_weight: bfloat16 [2048, 2048], P('sp', 'tp'), may hold values from -0.25 to 0.25
- norm_gain: bfloat16 [2048], replicated, may hold values from 0.099609375 to 1.8984375
- gate_weight: bfloat16 [2048, 7168], P('sp', 'tp'), may hold values from -0.125 to 0.125
- up_weight: bfloat16 [2048, 7168], P('sp', 'tp'), may hold values from -0.125 to 0.125
- down_weight: bfloat16 [7168, 2048], P('tp', 'sp'), may hold values from -0.125 to 0.125
Outputs:
- attended: bfloat16 [8192, 2048], P(('sp', 'tp'))
- layer_out: bfloat16 [8192, 2048], P(('sp', 'tp'))
The draws below stay inside these ranges and needn't reach their ends.
All inputs are finite; a program needn't handle non-finite values.
Results may differ from the reference program's by a relative error of at most 0.023.
Values may be sent and summed in bfloat16 or wider, within the bound.
A program may use at most 256 MiB of HBM per device.

```python
import jax
import jax.numpy as jnp
from jax import lax

D = 2048
FF = 7168
HEADS = 16
KV_HEADS = 8
HEAD_DIM = 128
TOK_DEV = 2048
SEQ = 8192
N_TP = 8


def shared_keys(key):
    sub_key = jax.random.fold_in(key, 5)
    base_draw = jnp.clip(jax.random.normal(sub_key, (SEQ, KV_HEADS * HEAD_DIM), jnp.float32), -5.0, 5.0)
    return base_draw


def draw_keys(key, part):
    return shared_keys(key).astype(jnp.bfloat16)


def draw_queries(key, part):
    sub_key = jax.random.fold_in(key, 9)
    base_draw = jnp.clip(2.5 * jax.random.normal(sub_key, (SEQ, HEADS * HEAD_DIM), jnp.float32), -15.0, 15.0)
    return base_draw.astype(jnp.bfloat16)


def level_of(own_key, dims, cuts, smallest, high):
    level = 1.0
    for position, shards_of in cuts:
        steps = jax.random.uniform(jax.random.fold_in(jax.random.fold_in(own_key, 6), position), (shards_of,), jnp.float32, smallest / len(cuts), high / len(cuts))
        level = level * jnp.repeat(jnp.exp(steps), dims[position] // shards_of).reshape((-1,) + (1,) * (len(dims) - 1 - position))
    return level


def scatter_about(stream_key, dims, width, most, shards=(), held_as=jnp.bfloat16):
    result = width * jax.random.normal(stream_key, dims, jnp.float32)
    if shards:
        result = result * level_of(stream_key, dims, shards, -0.22, 0.18)
    return jnp.clip(result, -most, most).astype(held_as)


def setup_inputs(seed: int = 0) -> dict:
    splits = jax.random.split(jax.random.key(seed), 10)
    return {
        "tokens": scatter_about(splits[0], (SEQ, D), 0.5, 3.0, ((0, 32),)),
        "queries": draw_queries(jax.random.fold_in(splits[9], 71), 0),
        "keys": draw_keys(jax.random.fold_in(splits[9], 71), 0),
        "values": scatter_about(splits[3], (SEQ, KV_HEADS * HEAD_DIM), 1.0, 6.0, ((0, 32),)),
        "out_weight": scatter_about(splits[4], (HEADS * HEAD_DIM, D), (HEADS * HEAD_DIM // 4) ** -0.5, 0.25, ((0, 4), (1, 8))),
        "norm_gain": jnp.clip(1.0 + 0.18 * jax.random.normal(splits[5], (D,), jnp.float32), 0.099609375, 1.8984375).astype(jnp.bfloat16),
        "gate_weight": scatter_about(splits[6], (D, FF), D ** -0.5, 0.125, ((0, 4), (1, 8))),
        "up_weight": scatter_about(splits[7], (D, FF), D ** -0.5, 0.125, ((0, 4), (1, 8))),
        "down_weight": scatter_about(splits[8], (FF, D), (FF // 4) ** -0.5, 0.125, ((0, 8), (1, 4))),
    }


def one_group(inputs):
    q_head, k_head, v_head = inputs
    seq_len = k_head.shape[0]
    group_size = q_head.shape[1]
    k_wide = k_head.astype(jnp.float32)
    v_wide = v_head.astype(jnp.float32)
    block_count = seq_len // TOK_DEV
    q_blocks = q_head.reshape(block_count, TOK_DEV, group_size, HEAD_DIM)
    starts = jnp.arange(block_count, dtype=jnp.int32) * TOK_DEV
    key_pos = jnp.arange(seq_len, dtype=jnp.int32)

    def one_block(pair):
        q_block, start = pair
        scores = jnp.einsum('qgd,kd->gqk', q_block.astype(jnp.float32), k_wide) * HEAD_DIM ** (-0.5)
        query_pos = start + jnp.arange(TOK_DEV, dtype=jnp.int32)
        causal = key_pos[None, :] <= query_pos[:, None]
        scores = jnp.where(causal[None, :, :], scores, -1e+30)
        row_peak = lax.optimization_barrier(jnp.max(scores, axis=-1, keepdims=True))
        exp_terms = jnp.exp(scores - row_peak)
        probs = (exp_terms / lax.optimization_barrier(jnp.sum(exp_terms, axis=-1, keepdims=True))).astype(jnp.bfloat16)
        mixed_out = jnp.einsum('gqk,kd->qgd', probs.astype(jnp.float32), v_wide)
        return mixed_out.astype(jnp.bfloat16)
    blocks_out = lax.map(one_block, (q_blocks, starts))
    return blocks_out.reshape(seq_len, group_size, HEAD_DIM)

def reference(tokens, queries, keys, values, out_weight, norm_gain, gate_weight, up_weight, down_weight):
    seq_len = tokens.shape[0]
    group_size = HEADS // KV_HEADS
    q_stack = jnp.transpose(queries.reshape(seq_len, KV_HEADS, group_size, HEAD_DIM), (1, 0, 2, 3))
    k_stack = jnp.transpose(keys.reshape(seq_len, KV_HEADS, HEAD_DIM), (1, 0, 2))
    v_stack = jnp.transpose(values.reshape(seq_len, KV_HEADS, HEAD_DIM), (1, 0, 2))
    grouped = lax.map(one_group, (q_stack, k_stack, v_stack))
    attn = jnp.transpose(grouped, (1, 0, 2, 3)).reshape(seq_len, HEADS * HEAD_DIM)
    projected = jnp.dot(attn, out_weight, preferred_element_type=jnp.float32)
    attended = (tokens.astype(jnp.float32) + projected).astype(jnp.bfloat16)
    attended_wide = attended.astype(jnp.float32)
    inverse_rms = lax.rsqrt(lax.optimization_barrier(jnp.mean(attended_wide * attended_wide, axis=1, keepdims=True)) + 1e-05)
    normed = (attended_wide * inverse_rms * norm_gain.astype(jnp.float32)).astype(jnp.bfloat16)
    gate_sum = jnp.dot(normed, gate_weight, preferred_element_type=jnp.float32)
    up_sum = jnp.dot(normed, up_weight, preferred_element_type=jnp.float32)
    hidden = (jax.nn.silu(gate_sum) * up_sum).astype(jnp.bfloat16)
    block_width = FF // N_TP
    hidden_blocks = jnp.transpose(hidden.reshape(seq_len, N_TP, block_width), (1, 0, 2))
    down_blocks = down_weight.reshape(N_TP, block_width, D)

    def add_block(total, pair):
        hidden_block, down_block = pair
        partial_value = jnp.dot(hidden_block, down_block, preferred_element_type=jnp.float32).astype(jnp.bfloat16)
        partial_value = lax.optimization_barrier(partial_value)
        return (total + partial_value.astype(jnp.float32), None)
    ffn_part, _ = lax.scan(add_block, jnp.zeros((seq_len, D), jnp.float32), (hidden_blocks, down_blocks))
    layer_out = (attended_wide + ffn_part).astype(jnp.bfloat16)
    return (attended, layer_out)
```

```python
import functools
import math

import jax
import jax.numpy as jnp
from jax import lax
from jax.experimental import pallas as pl
from jax.experimental.pallas import tpu as pltpu
from jax.sharding import PartitionSpec as P

HEAD_DIM = 128
KEY_CHUNK = 512
LOG2_SCALE = HEAD_DIM ** (-0.5) * math.log2(math.e)
norm_eps = 1e-05


def attend_kernel(
    shift, sp_count, segment_len, kv_local, where_ref, q_ref, kv_ref, out_ref, qt_ref, acc_ref
):
    rows = q_ref.shape[0]
    group = q_ref.shape[1] // (kv_local * HEAD_DIM)
    width = group * rows
    sp_me, tp_me = where_ref[0], where_ref[1]
    start = lax.rem(sp_me + shift, sp_count) * segment_len + tp_me * rows
    for g in range(kv_local):
        for h in range(group):
            head = g * group + h
            qt_ref[g, :, h * rows : (h + 1) * rows] = q_ref[
                :, head * HEAD_DIM : (head + 1) * HEAD_DIM
            ].T
    acc_ref[...] = jnp.zeros_like(acc_ref)

    def step(chunk, carry, masked):
        first = chunk * KEY_CHUNK
        segment = first // segment_len
        slot = lax.rem(sp_me - segment + sp_count, sp_count)
        offset = pl.multiple_of(
            slot * segment_len + first - segment * segment_len, KEY_CHUNK
        )
        scores = []
        for g in range(kv_local):
            k = kv_ref[pl.ds(offset, KEY_CHUNK), g * HEAD_DIM : (g + 1) * HEAD_DIM]
            s = jnp.dot(k, qt_ref[g], preferred_element_type=jnp.float32)
            if masked:
                key_pos = first + lax.broadcasted_iota(jnp.int32, (KEY_CHUNK, width), 0)
                lane = lax.broadcasted_iota(jnp.int32, (KEY_CHUNK, width), 1)
                s = jnp.where(key_pos <= start + lax.rem(lane, rows), s, -1e30)
            scores.append(s)
        result = []
        for g in range(kv_local):
            peak, total = carry[g]
            s = scores[g]
            new_peak = jnp.maximum(peak, jnp.max(s, axis=0, keepdims=True))
            p = jnp.exp2((s - new_peak) * LOG2_SCALE)
            fade = jnp.exp2((peak - new_peak) * LOG2_SCALE)
            total = total * fade + jnp.sum(p, axis=0, keepdims=True)
            v_at = (kv_local + g) * HEAD_DIM
            v = kv_ref[pl.ds(offset, KEY_CHUNK), v_at : v_at + HEAD_DIM]
            acc_ref[g] = acc_ref[g] * fade + lax.dot_general(
                v,
                p.astype(jnp.bfloat16),
                (((0,), (0,)), ((), ())),
                preferred_element_type=jnp.float32,
            )
            result.append((new_peak, total))
        return tuple(result)

    carry = tuple(
        (jnp.full((1, width), -1e30, jnp.float32), jnp.zeros((1, width), jnp.float32))
        for _ in range(kv_local)
    )
    whole_chunks = start // KEY_CHUNK
    carry = lax.fori_loop(0, whole_chunks, lambda i, c: step(i, c, False), carry)
    carry = step(whole_chunks, carry, True)
    for g in range(kv_local):
        mixed = (acc_ref[g] / carry[g][1]).astype(jnp.bfloat16)
        for h in range(group):
            head = g * group + h
            out_ref[:, head * HEAD_DIM : (head + 1) * HEAD_DIM] = mixed[
                :, h * rows : (h + 1) * rows
            ].T


def attend(shift, sp_count, segment_len, where, q_block, all_kv):
    rows, q_width = q_block.shape
    kv_local = all_kv.shape[1] // (2 * HEAD_DIM)
    width = q_width // (kv_local * HEAD_DIM) * rows
    keys = all_kv.shape[0]
    return pl.pallas_call(
        functools.partial(attend_kernel, shift, sp_count, segment_len, kv_local),
        out_shape=jax.ShapeDtypeStruct((rows, q_width), jnp.bfloat16),
        in_specs=[
            pl.BlockSpec(memory_space=pltpu.SMEM),
            pl.BlockSpec(memory_space=pltpu.VMEM),
            pl.BlockSpec(memory_space=pltpu.VMEM),
        ],
        out_specs=pl.BlockSpec(memory_space=pltpu.VMEM),
        scratch_shapes=[
            pltpu.VMEM((kv_local, HEAD_DIM, width), jnp.bfloat16),
            pltpu.VMEM((kv_local, HEAD_DIM, width), jnp.float32),
        ],
        cost_estimate=pl.CostEstimate(
            flops=2 * rows * q_width * keys,
            bytes_accessed=all_kv.size * 2,
            transcendentals=rows * q_width // HEAD_DIM * keys // 2,
        ),
        compiler_params=pltpu.CompilerParams(vmem_limit_bytes=40 * 1024 * 1024),
    )(where, q_block, all_kv)


def turn(array, count, shift):
    return lax.ppermute(array, "sp", [(i, (i + shift) % count) for i in range(count)])


def gather_ring(piece, count, me, axis):
    size = piece.shape[axis]
    shape = list(piece.shape)
    shape[axis] = size * count
    full = jnp.zeros(shape, piece.dtype)

    def put(full, block, owner, extra=0):
        at = [0, 0]
        at[axis] = lax.rem(owner + count, count) * size
        at[0] = at[0] + extra
        return lax.dynamic_update_slice(full, block, at)

    full = put(full, piece, me)
    up = down = piece
    for step in range(1, (count + 1) // 2):
        up, down = turn(up, count, 1), turn(down, count, -1)
        full = put(full, up, me - step)
        full = put(full, down, me + step)
    if count % 2 == 0:
        half = piece.shape[0] // 2
        far = me + count // 2
        full = put(full, turn(up[:half], count, 1), far)
        full = put(full, turn(down[half:], count, -1), far, half)
    return full


def shards(
    tokens, queries, keys, values, out_weight, norm_gain, gate_weight, up_weight, down_weight
):
    shard_rows = tokens.shape[0]
    sp_count = lax.axis_size("sp")
    tp_count = lax.axis_size("tp")
    sp_me = lax.axis_index("sp")
    tp_me = lax.axis_index("tp")
    segment_len = shard_rows * tp_count

    def part(array, shift):
        size = array.shape[1] // sp_count
        block = lax.rem(sp_me + shift, sp_count)
        return lax.dynamic_slice_in_dim(array, block * size, size, 1)

    kv_slots, q_slots = [], []
    for shift in range(sp_count):
        kv = jnp.concatenate([part(keys, shift), part(values, shift)], axis=1)
        kv_slots.append(turn(kv, sp_count, shift) if shift else kv)
    for shift in range(sp_count):
        q = part(queries, shift)
        q_slots.append(turn(q, sp_count, shift) if shift else q)
    kv_stack = jnp.stack(kv_slots)
    all_kv = lax.all_gather(kv_stack, "tp", axis=1, tiled=True)
    all_kv = all_kv.reshape(sp_count * segment_len, -1)
    wo_full = lax.all_gather(out_weight, "tp", axis=1, tiled=True)
    (gate_weight, up_weight, down_weight), q_slots = lax.optimization_barrier(
        ((gate_weight, up_weight, down_weight), tuple(q_slots))
    )
    gate_full = gather_ring(gate_weight, sp_count, sp_me, 0)
    up_full = gather_ring(up_weight, sp_count, sp_me, 0)
    down_full = gather_ring(down_weight, sp_count, sp_me, 1)

    where = jnp.stack([sp_me, tp_me]).astype(jnp.int32)
    attn_part = None
    received = []
    for shift in list(range(1, sp_count)) + [0]:
        q = q_slots[(sp_count - shift) % sp_count]
        attn = attend(shift, sp_count, segment_len, where, q, all_kv)
        share = jnp.dot(attn, wo_full, preferred_element_type=jnp.float32)
        share = share.astype(jnp.bfloat16)
        received.append(turn(share, sp_count, shift) if shift else share)
    attn_part = sum(block.astype(jnp.float32) for block in received)
    attended = (tokens.astype(jnp.float32) + attn_part).astype(jnp.bfloat16)
    attended_wide = attended.astype(jnp.float32)
    inverse_rms = lax.rsqrt(
        jnp.mean(attended_wide * attended_wide, axis=1, keepdims=True) + norm_eps
    )
    normed = (attended_wide * inverse_rms * norm_gain.astype(jnp.float32)).astype(jnp.bfloat16)

    halves = 2
    half = shard_rows // halves
    outs = []
    for i in range(halves):
        rows = lax.all_gather(normed[i * half : (i + 1) * half], "tp", axis=0, tiled=True)
        gate_sum = jnp.dot(rows, gate_full, preferred_element_type=jnp.float32)
        up_sum = jnp.dot(rows, up_full, preferred_element_type=jnp.float32)
        hidden = (jax.nn.silu(gate_sum) * up_sum).astype(jnp.bfloat16)
        share = jnp.dot(hidden, down_full, preferred_element_type=jnp.float32)
        outs.append(
            lax.psum_scatter(
                share.astype(jnp.bfloat16), "tp", scatter_dimension=0, tiled=True
            ).astype(jnp.float32)
        )
    layer_out = (attended_wide + jnp.concatenate(outs, axis=0)).astype(jnp.bfloat16)
    return (attended, layer_out)


def solution(mesh):
    return jax.shard_map(
        shards,
        mesh=mesh,
        in_specs=(
            P(("sp", "tp"), None),
            P(("sp", "tp"), None),
            P(("sp", "tp"), None),
            P(("sp", "tp"), None),
            P("sp", "tp"),
            P(),
            P("sp", "tp"),
            P("sp", "tp"),
            P("tp", "sp"),
        ),
        out_specs=(P(("sp", "tp"), None), P(("sp", "tp"), None)),
        check_vma=False,
    )
```
